32 devices in a mesh: outer: 8 (over z, x), inner: 4 (over y, core).
Axes of the slice: x: 2, y: 2, z: 4, core: 2. Of those that a mesh axis runs over, the one named last changes fastest.
Arguments:
- queries: bfloat16 [8192, 1024], P(('outer', 'inner')), may hold values from -10 to 10
- keys: bfloat16 [8192, 256], P(('outer', 'inner')), may hold values from -10 to 10
- values: bfloat16 [8192, 256], P(('outer', 'inner')), may hold values from -18 to 18
- pool_fine: float32 [16, 8], replicated, may hold values from -1.5 to 1.5
- pool_coarse: float32 [8, 8], replicated, may hold values from -2 to 2
- gain: float32 [1024], replicated, may hold values from 0.5 to 1.5
Outputs:
- normed: bfloat16 [8192, 1024], P(('outer', 'inner'))
The draws below stay inside these ranges and needn't reach their ends.
All inputs are finite; a program needn't handle non-finite values.
Results may differ from the reference program's by a relative error of at most 0.008.
Values may be sent and summed in bfloat16 or wider, within the bound.
A program may use at most 64 MiB of HBM per device.

```python
import jax
import jax.numpy as jnp
from jax import lax

HQ = 16
KVH = 4
HD = 64
BLOCK = 512
FINE = 16
RATIO = 8
D = 1024
COARSE = 128
GROUP = 1024
TOKENS = 8192


def joint_draw(key):
    base = jax.random.fold_in(key, 7)
    draw_q, draw_k = jax.random.split(base, 2)
    width_q = HQ * HD
    width_k = KVH * HD
    queries = jnp.clip(jax.random.normal(draw_q, (TOKENS, width_q), jnp.float32), -6.0, 6.0)
    keys = jnp.clip(jax.random.normal(draw_k, (TOKENS, width_k), jnp.float32), -6.0, 6.0)
    return (queries, keys)


def draw_queries(key, part):
    return joint_draw(key)[0].astype(jnp.bfloat16)


def draw_keys(key, part):
    return joint_draw(key)[1].astype(jnp.bfloat16)


def draw_values(key, part):
    base = jax.random.fold_in(key, 11)
    draw_v = jax.random.fold_in(base, 0)
    drawn = jnp.clip(jax.random.normal(draw_v, (TOKENS, KVH * HD), jnp.float32), -6.0, 6.0)
    return drawn.astype(jnp.bfloat16)


def noise(stream_key, extent, width, reach, held_as=jnp.bfloat16):
    entries = jax.random.normal(stream_key, extent, jnp.float32) * width
    return jnp.minimum(jnp.maximum(entries, -reach), reach).astype(held_as)


def setup_inputs(seed: int = 0) -> dict:
    key_list = jax.random.split(jax.random.key(seed), 7)
    return {
        "queries": draw_queries(jax.random.fold_in(key_list[6], 71), 0),
        "keys": draw_keys(jax.random.fold_in(key_list[6], 71), 0),
        "values": draw_values(jax.random.fold_in(key_list[6], 71), 0),
        "pool_fine": noise(key_list[3], (FINE, 2 * KVH), FINE ** -0.5, 1.5, jnp.float32),
        "pool_coarse": noise(key_list[4], (RATIO, 2 * KVH), RATIO ** -0.5, 2.0, jnp.float32),
        "gain": jnp.clip(1.0 + 0.1 * jax.random.normal(key_list[5], (D,), jnp.float32), 0.5, 1.5),
    }


EPSILON = 1e-06
MASKED_SCORE = -1e+30

def summarize(source, pooling, factor):
    amount = source.shape[0] // factor
    shaped = source.astype(jnp.float32).reshape(amount, factor, 2, KVH, HD)
    weights = pooling.astype(jnp.float32).reshape(factor, 2, KVH)
    pooled = jnp.einsum('mjskd,jsk->mskd', shaped, weights, precision=lax.Precision.HIGHEST)
    return pooled.reshape(amount, 2 * KVH * HD).astype(jnp.bfloat16)

def reference(queries, keys, values, pool_fine, pool_coarse, gain):
    paired = jnp.concatenate([keys, values], axis=1)
    fine_all = summarize(paired, pool_fine, FINE)
    coarse_all = summarize(fine_all, pool_coarse, RATIO)
    padded = jnp.pad(paired, ((BLOCK, BLOCK), (0, 0)))
    fine_group = GROUP // FINE
    coarse_pos = jnp.arange(TOKENS // COARSE, dtype=jnp.int32) * COARSE
    kv_width = KVH * HD

    def one_block(block_idx):
        first_row = (block_idx * BLOCK).astype(jnp.int32)
        query_rows = lax.dynamic_slice_in_dim(queries, first_row, BLOCK, 0)
        near = lax.dynamic_slice_in_dim(padded, first_row, 3 * BLOCK, 0)
        near_pos = first_row - BLOCK + jnp.arange(3 * BLOCK, dtype=jnp.int32)
        near_ok = (near_pos >= 0) & (near_pos < TOKENS)
        group_idx = (first_row // GROUP).astype(jnp.int32)
        fine_rows = lax.dynamic_slice_in_dim(fine_all, (group_idx * fine_group).astype(jnp.int32), fine_group, 0)
        fine_pos = group_idx * GROUP + jnp.arange(fine_group, dtype=jnp.int32) * FINE
        fine_ok = jnp.abs(fine_pos // BLOCK - block_idx) > 1
        coarse_ok = (coarse_pos // GROUP != group_idx) & (jnp.abs(coarse_pos // BLOCK - block_idx) > 1)
        keyset = jnp.concatenate([near, fine_rows, coarse_all], axis=0)
        allowed = jnp.concatenate([near_ok, fine_ok, coarse_ok])
        amount = keyset.shape[0]
        key_heads = keyset[:, :kv_width].astype(jnp.float32).reshape(amount, KVH, HD)
        value_heads = keyset[:, kv_width:].astype(jnp.float32).reshape(amount, KVH, HD)
        query_heads = query_rows.astype(jnp.float32).reshape(BLOCK, KVH, HQ // KVH, HD)
        scores = jnp.einsum('qgrd,kgd->grqk', query_heads, key_heads, precision=lax.Precision.HIGHEST) * HD ** (-0.5)
        scores = jnp.where(allowed, scores, MASKED_SCORE)
        peak = lax.optimization_barrier(jnp.max(scores, axis=3, keepdims=True))
        expon = jnp.where(allowed, jnp.exp(scores - peak), 0.0)
        totals = lax.optimization_barrier(jnp.sum(expon, axis=3))
        rounded = lax.optimization_barrier(expon.astype(jnp.bfloat16)).astype(jnp.float32)
        blended = jnp.einsum('grqk,kgd->qgrd', rounded, value_heads, precision=lax.Precision.HIGHEST)
        attended = blended / jnp.transpose(totals, (2, 0, 1))[..., None]
        return attended.reshape(BLOCK, HQ * HD)
    attended = lax.map(one_block, jnp.arange(TOKENS // BLOCK, dtype=jnp.int32)).reshape(TOKENS, HQ * HD)
    rescale = lax.rsqrt(lax.optimization_barrier(jnp.mean(attended * attended, axis=1, keepdims=True)) + EPSILON)
    return (attended * rescale * gain).astype(jnp.bfloat16)
```

```python
import contextlib
import functools
import math

import jax
import jax.numpy as jnp
from jax import lax
from jax.experimental import pallas as pl
from jax.experimental.pallas import tpu as pltpu
from jax.sharding import PartitionSpec as P

HQ = 16
KVH = 4
HD = 64
BLOCK = 512
FINE = 16
RATIO = 8
COARSE = 128

EPSILON = 1e-06
LANES = 128
ONES = 16
UNITS = 4
MESH = pl.DeviceIdType.MESH
BF16 = jnp.bfloat16
F32 = jnp.float32
FACTOR = HD ** (-0.5) * math.log2(math.e)


def scope(name):
    return contextlib.nullcontext()


def kernel(
    outer_count, inner_count, use_fine,
    q_hbm, k_hbm, v_hbm, pf_hbm, pc_hbm, out_ref,
    q_ref, k_ref, v_ref, pf_ref, pc_ref, in_sems,
    q_all, queries_t, values_t, own_k, own_v, mate_k, mate_v, other_k, other_v,
    score_ref, weight_ref, peaks, sums, peak_now, decay_next, decay_now,
    fine_send, fine_all, coarse_send, coarse_pad, coarse_all,
    att_send,
    q_ss, q_rs, own_ss, own_rs, mate_ss, mate_rs, other_ss, other_rs,
    fine_ss, fine_rs, cg_ss, cg_rs, co_ss, co_rs, att_ss, att_rs,
):
    tok = q_ref.shape[0]
    ranks = BLOCK // tok
    kv_width = KVH * HD
    share = kv_width // ranks
    q_share = HQ * HD // ranks
    tiles = q_share // LANES
    heads = q_share // HD
    kv_local = share // HD
    heads_kv = heads // kv_local
    fine_dev = tok // FINE
    coarse_dev = tok // COARSE
    group_tok = tok * inner_count
    fine_amount = group_tok // FINE if use_fine else 0
    coarse_group = inner_count * coarse_dev
    coarse_amount = outer_count * coarse_group
    blocks = outer_count * inner_count // ranks
    levels = outer_count.bit_length() - 1

    o_me = lax.axis_index("outer")
    i_me = lax.axis_index("inner")
    linear = o_me * inner_count + i_me
    block = linear // ranks
    rank = lax.rem(linear, ranks)
    odd = lax.rem(block, 2)
    mate = block + 1 - 2 * odd
    relay_from = block - 2 + 4 * odd
    relay_to = block + 2 - 4 * odd
    has_other = (relay_from >= 0) & (relay_from < blocks)
    has_next = (relay_to >= 0) & (relay_to < blocks)

    def at_rank(which_block, rel):
        target_rank = lax.rem(rank + rel, ranks)
        spot = which_block * ranks + target_rank
        return (spot // inner_count, lax.rem(spot, inner_count)), target_rank

    inner_peers = [lax.rem(i_me + rel, inner_count) for rel in range(1, inner_count)]
    outer_peers = [
        o_me + 2 ** level * (1 - 2 * lax.rem(o_me // 2 ** level, 2)) for level in range(levels)]

    loads = [
        pltpu.make_async_copy(src, dst, in_sems.at[n])
        for n, (src, dst) in enumerate((
            (k_hbm, k_ref), (q_hbm, q_ref), (v_hbm, v_ref), (pf_hbm, pf_ref), (pc_hbm, pc_ref)))
    ]
    for load in loads:
        load.start()

    barrier = pltpu.get_barrier_semaphore()

    def greet(device):
        pl.semaphore_signal(barrier, inc=1, device_id=device, device_id_type=MESH)

    for peer in inner_peers:
        greet((o_me, peer))
    for peer in outer_peers:
        greet((peer, i_me))
    for which in (relay_from, relay_to):
        greet(at_rank(lax.rem(which + blocks, blocks), 0)[0])

    def remote(src, dst, send_sem, recv_sem, device):
        return pltpu.make_async_remote_copy(
            src_ref=src, dst_ref=dst, send_sem=send_sem, recv_sem=recv_sem,
            device_id=device, device_id_type=MESH,
        )

    def cols(index, width):
        return pl.ds(pl.multiple_of(index * width, LANES), width)

    def k_at(ref, slot):
        return ref.at[pl.ds(slot * tok, tok)]

    def v_at(ref, slot):
        return ref.at[:, pl.ds(0, HD), pl.ds(slot * tok, tok)]

    own_k_copies, own_q_copies, own_v_copies = [], [], []
    for rel in range(1, ranks):
        device, target = at_rank(block, rel)
        slot = ranks - rel
        own_k_copies.append(remote(
            k_ref.at[:, cols(target, share)], k_at(own_k, slot),
            own_ss.at[0, slot], own_rs.at[0, slot], device))
        own_q_copies.append(remote(
            q_ref.at[:, cols(target, q_share)], q_all.at[slot],
            q_ss.at[slot], q_rs.at[slot], device))
        own_v_copies.append(remote(
            values_t.at[target], v_at(own_v, slot),
            own_ss.at[1, slot], own_rs.at[1, slot], device))
    mate_k_copies, mate_v_copies = [], []
    for rel in range(ranks):
        device, target = at_rank(mate, rel)
        slot = (ranks - rel) % ranks
        mate_k_copies.append(remote(
            k_ref.at[:, cols(target, share)], k_at(mate_k, slot),
            mate_ss.at[0, slot], mate_rs.at[0, slot], device))
        mate_v_copies.append(remote(
            values_t.at[target], v_at(mate_v, slot),
            mate_ss.at[1, slot], mate_rs.at[1, slot], device))
    next_device = at_rank(relay_to, 0)[0]
    relay_k_copies = [remote(
        k_at(mate_k, slot), k_at(other_k, slot),
        other_ss.at[0, slot], other_rs.at[0, slot], next_device) for slot in range(ranks)]
    relay_v_copies = [remote(
        v_at(mate_v, slot), v_at(other_v, slot),
        other_ss.at[1, slot], other_rs.at[1, slot], next_device) for slot in range(ranks)]
    group_copies, fine_copies = [], []
    for n, peer in enumerate(inner_peers):
        peer_rank = lax.rem(peer, ranks)
        group_copies.append(remote(
            coarse_send.at[peer_rank], coarse_pad.at[i_me],
            cg_ss.at[n], cg_rs.at[n], (o_me, peer)))
        if use_fine:
            fine_copies.append(remote(
                fine_send.at[peer_rank], fine_all.at[i_me],
                fine_ss.at[n], fine_rs.at[n], (o_me, peer)))
    outer_copies = []
    for level, peer in enumerate(outer_peers):
        size = 2 ** level
        span = pl.ds(o_me // size * size, size)
        outer_copies.append(remote(
            coarse_all.at[span], coarse_all.at[span], co_ss.at[level], co_rs.at[level],
            (peer, i_me)))

    queries_t[...] = jnp.zeros(queries_t.shape, BF16)
    for ref in (own_v, mate_v, other_v):
        ref[:, HD:, :] = jnp.ones((kv_local, ONES, ref.shape[2]), BF16)

    with scope("wk"):
        loads[0].wait()
    with scope("wbar"):
        pl.semaphore_wait(barrier, inner_count - 1 + levels + 2)
    for copy in own_k_copies + mate_k_copies:
        copy.start()
    with scope("wq"):
        loads[1].wait()
    for copy in own_q_copies:
        copy.start()
    with scope("wv"):
        for load in loads[2:]:
            load.wait()

    def spread(pool):
        rows = pool.shape[0]
        return jnp.concatenate(
            [jnp.broadcast_to(pool[:, n:n + 1], (rows, HD)) for n in range(2 * KVH)], axis=1)

    pf = spread(pf_ref[...].T)
    pc = spread(pc_ref[...])
    paired = jnp.concatenate([k_ref[...], v_ref[...]], axis=1).astype(F32)
    fine = jnp.sum(paired.reshape(fine_dev, FINE, 2 * kv_width) * pf[None], axis=1).astype(BF16)
    fine_wide = fine.astype(F32)
    coarse_wide = jnp.sum(
        fine_wide.reshape(coarse_dev, RATIO, 2 * kv_width) * pc[None], axis=1
    ).astype(BF16).astype(F32)
    padded = coarse_send.shape[1]
    for n in range(ranks):
        k_cols = slice(n * share, (n + 1) * share)
        v_cols = slice(kv_width + n * share, kv_width + (n + 1) * share)
        if use_fine:
            fine_send[n] = jnp.concatenate([fine[:, k_cols], fine[:, v_cols]], axis=1)
        parts = [coarse_wide[:, k_cols], coarse_wide[:, v_cols]]
        if padded > 2 * coarse_dev:
            parts.append(jnp.zeros((padded - 2 * coarse_dev, share), F32))
        coarse_send[n] = jnp.concatenate(parts, axis=0)
    coarse_pad[i_me] = coarse_send[rank]
    if use_fine:
        fine_all[i_me] = fine_send[rank]
    for copy in group_copies:
        copy.start()
    turned = v_ref[...].T
    for n in range(ranks):
        for x in range(kv_local):
            row = n * share + x * HD
            values_t[n, x] = turned[row:row + HD]
    for copy in own_v_copies + mate_v_copies + fine_copies:
        copy.start()

    def arrange(part, tile_of):
        for x in range(tiles):
            turned = tile_of(x).T
            low = (2 * x // heads_kv) * HD
            for y in range(2):
                queries_t[part * heads + 2 * x + y, low:low + HD, :] = turned[y * HD:(y + 1) * HD]

    def score(unit, n, k_set, first):
        amount = k_set.shape[0]
        scores = jnp.dot(k_set, queries_t[unit], preferred_element_type=F32)
        peak = jnp.max(scores, axis=0, keepdims=True)
        if not first:
            before = peaks[unit]
            peak = jnp.maximum(peak, before)
            decay_next[n] = jnp.exp2((before - peak) * FACTOR)
        score_ref[n, 0:amount, :] = scores
        peaks[unit] = peak
        peak_now[n] = peak

    def weigh(n, amount, first):
        weight_ref[n, 0:amount, :] = jnp.exp2(
            (score_ref[n, 0:amount, :] - peak_now[n]) * FACTOR).astype(BF16)
        if not first:
            decay_now[n] = decay_next[n]

    def blend(unit, n, v_set, first):
        amount = v_set.shape[1]
        blended = jnp.dot(v_set, weight_ref[n, 0:amount, :], preferred_element_type=F32)
        sums[unit] = blended if first else sums[unit] * decay_now[n] + blended

    def run(groups, after=None):
        count = len(groups)
        for step in range(count + 2):
            if step >= 2:
                units, _, v_of, amount, first = groups[step - 2]
                for n, unit in enumerate(units):
                    blend(unit, n, v_of(unit % heads // heads_kv), first)
            if 1 <= step < count + 1:
                units, _, _, amount, first = groups[step - 1]
                for n in range(len(units)):
                    weigh(n, amount, first)
            if step < count:
                units, k_of, _, amount, first = groups[step]
                k_set = k_of()
                for n, unit in enumerate(units):
                    score(unit, n, k_set, first)
            if after is not None and step >= 2:
                after(step - 2)

    def units_of(part):
        base = part * heads
        return [list(range(base + n, base + n + UNITS)) for n in range(0, heads, UNITS)]

    def groups_of(parts, k_ref_, v_ref_, span, first):
        amount = span.stop - span.start
        return [
            (units, lambda: k_ref_[span, :], lambda g: v_ref_[g, :, span], amount, first)
            for part in parts for units in units_of(part)]

    with scope("prep0"):
        own_k[0:tok, :] = k_ref[:, cols(rank, share)]
        own_v[:, 0:HD, 0:tok] = values_t[rank]
        arrange(0, lambda x: q_ref[:, cols(rank * tiles + x, LANES)])
    with scope("own0"):
        run(groups_of([0], own_k, own_v, slice(0, tok), True))

    with scope("w_own"):
        for copy in own_k_copies + own_q_copies + own_v_copies:
            copy.wait_recv()
    with scope("prep1"):
        for slot in range(1, ranks):
            arrange(slot, lambda x: q_all[slot, :, x * LANES:(x + 1) * LANES])
    with scope("own1"):
        run(groups_of(range(1, ranks), own_k, own_v, slice(0, BLOCK), True)
            + groups_of([0], own_k, own_v, slice(tok, BLOCK), False))

    with scope("w_group"):
        for copy in group_copies:
            copy.wait_recv()
    for n in range(inner_count):
        rows = slice(n * coarse_dev, (n + 1) * coarse_dev)
        lower = slice(coarse_group + n * coarse_dev, coarse_group + (n + 1) * coarse_dev)
        coarse_all[o_me, rows, :] = coarse_pad[n, 0:coarse_dev, :]
        coarse_all[o_me, lower, :] = coarse_pad[n, coarse_dev:2 * coarse_dev, :]

    def climb(level):
        if level > 0:
            outer_copies[level - 1].wait_recv()
        if level < levels:
            outer_copies[level].start()

    climb(0)
    with scope("w_mk"):
        for copy in mate_k_copies:
            copy.wait_recv()

    @pl.when(has_next)
    def _():
        for copy in relay_k_copies:
            copy.start()

    with scope("climb1"):
        climb(1)
    with scope("w_mv"):
        for copy in mate_v_copies:
            copy.wait_recv()

    @pl.when(has_next)
    def _():
        for copy in relay_v_copies:
            copy.start()

    with scope("climb2"):
        for level in range(2, levels):
            climb(level)
    with scope("mate"):
        run(groups_of(range(ranks), mate_k, mate_v, slice(0, BLOCK), False))

    with scope("climb3"):
        climb(levels)
    with scope("far"):
        far = fine_amount + coarse_amount
        k_far = coarse_all[:, 0:coarse_group, :].reshape(coarse_amount, share)
        v_far = coarse_all[:, coarse_group:, :].reshape(coarse_amount, share)
        if use_fine:
            for copy in fine_copies:
                copy.wait_recv()
            fine_rows = fine_all[...].reshape(fine_amount, 2 * share).astype(F32)
            k_far = jnp.concatenate([fine_rows[:, :share], k_far], axis=0)
            v_far = jnp.concatenate([fine_rows[:, share:], v_far], axis=0)

        def reachable(shape, axis):
            spot = lax.broadcasted_iota(jnp.int32, shape, axis)
            fine_pos = o_me * group_tok + spot * FINE
            coarse_pos = (spot - fine_amount) * COARSE
            position = jnp.where(spot < fine_amount, fine_pos, coarse_pos)
            distance = jnp.abs(lax.div(position, BLOCK) - block)
            outside = (spot < fine_amount) | (lax.div(position, group_tok) != o_me)
            return (distance > 1) & outside

        stand_in = own_k[0:16, :].astype(F32)[0:1, :]
        other_k[BLOCK:, :] = jnp.where(
            reachable((far, share), 0), k_far, jnp.broadcast_to(stand_in, (far, share))).astype(BF16)
        open_cols = reachable((HD, far), 1)
        turned = v_far.T
        for x in range(kv_local):
            other_v[x, 0:HD, BLOCK:] = jnp.where(
                open_cols, turned[x * HD:(x + 1) * HD, :], 0.0).astype(BF16)
            other_v[x, HD:, BLOCK:] = open_cols[0:ONES].astype(F32).astype(BF16)

    @pl.when(has_other)
    def _():
        with scope("w_other"):
            for copy in relay_k_copies + relay_v_copies:
                copy.wait_recv()

    @pl.when(jnp.logical_not(has_other))
    def _():
        other_k[0:BLOCK, :] = own_k[...]
        other_v[:, :, 0:BLOCK] = jnp.zeros((kv_local, HD + ONES, BLOCK), BF16)

    def finish(unit):
        total = sums[unit]
        return total[0:HD] / total[HD:HD + 1]

    def att_copy(part, at):
        device, _ = at_rank(block, part)
        slot = ranks - part - 1
        row = pl.multiple_of(rank * q_share + at * UNITS * HD, HD)
        return remote(att_send.at[part - 1, pl.ds(at * UNITS * HD, UNITS * HD)],
                      out_ref.at[pl.ds(row, UNITS * HD)],
                      att_ss.at[slot, at], att_rs.at[slot, at], device)

    order = list(range(1, ranks)) + [0]
    per_part = heads // UNITS

    def after(index):
        part, at = order[index // per_part], index % per_part
        for n in range(UNITS):
            head = at * UNITS + n
            attended = finish(part * heads + head)
            if part:
                att_send[part - 1, head * HD:(head + 1) * HD, :] = attended
            else:
                out_ref[pl.ds(pl.multiple_of(rank * q_share + head * HD, HD), HD), :] = attended
        if part:
            att_copy(part, at).start()

    with scope("other"):
        run(groups_of(order, other_k, other_v, slice(0, BLOCK + far), False), after)

    with scope("w_att"):
        for part in range(1, ranks):
            for at in range(per_part):
                att_copy(part, at).wait_recv()

    with scope("w_send"):
        for copy in (own_k_copies + own_q_copies + own_v_copies + mate_k_copies + mate_v_copies
                     + group_copies + fine_copies + outer_copies):
            copy.wait_send()

        @pl.when(has_next)
        def _():
            for copy in relay_k_copies + relay_v_copies:
                copy.wait_send()

        for part in range(1, ranks):
            for at in range(per_part):
                att_copy(part, at).wait_send()


def norm_kernel(attended_ref, gain_ref, out_ref):
    attended = attended_ref[...]
    rescale = lax.rsqrt(jnp.mean(attended * attended, axis=0, keepdims=True) + EPSILON)
    out_ref[...] = ((attended * rescale).T * gain_ref[...]).astype(BF16)


def local(outer_count, inner_count, queries, keys, values, pool_fine, pool_coarse, gain):
    tok = queries.shape[0]
    ranks = BLOCK // tok
    share = KVH * HD // ranks
    kv_local = share // HD
    q_share = HQ * HD // ranks
    heads = q_share // HD
    group_tok = tok * inner_count
    use_fine = group_tok > 2 * BLOCK
    far = (group_tok // FINE if use_fine else 0) + outer_count * group_tok // COARSE
    coarse_dev = tok // COARSE
    padded = -(-2 * coarse_dev // 8) * 8
    levels = outer_count.bit_length() - 1
    assert ranks >= 2 and BLOCK % tok == 0 and kv_local == 2 and share == LANES
    assert inner_count % (2 * ranks) == 0 and outer_count == 2 ** levels
    dma = pltpu.SemaphoreType.DMA
    vmem = pltpu.VMEM
    units = ranks * heads
    pair = lambda: dma((2, ranks))
    k_set = lambda amount: vmem((amount, share), BF16)
    v_set = lambda amount: vmem((kv_local, HD + ONES, amount), BF16)
    line = lambda: vmem((UNITS, 1, tok), F32)
    attended = pl.pallas_call(
        functools.partial(kernel, outer_count, inner_count, use_fine),
        out_shape=jax.ShapeDtypeStruct((HQ * HD, tok), F32),
        in_specs=[pl.BlockSpec(memory_space=pltpu.HBM)] * 5,
        out_specs=pl.BlockSpec(memory_space=pltpu.VMEM),
        scratch_shapes=[
            vmem(queries.shape, BF16), vmem(keys.shape, BF16), vmem(values.shape, BF16),
            vmem(pool_fine.shape[::-1], F32), vmem(pool_coarse.shape, F32), dma((5,)),
            vmem((ranks, tok, q_share), BF16),
            vmem((units, share, tok), BF16),
            vmem((ranks, kv_local, HD, tok), BF16),
            k_set(BLOCK), v_set(BLOCK), k_set(BLOCK), v_set(BLOCK),
            k_set(BLOCK + far), v_set(BLOCK + far),
            vmem((UNITS, BLOCK + far, tok), F32),
            vmem((UNITS, BLOCK + far, tok), BF16),
            vmem((units, 1, tok), F32),
            vmem((units, HD + ONES, tok), F32),
            line(), line(), line(),
            vmem((ranks, tok // FINE, 2 * share), BF16),
            vmem((inner_count, tok // FINE, 2 * share), BF16),
            vmem((ranks, padded, share), F32),
            vmem((inner_count, padded, share), F32),
            vmem((outer_count, 2 * inner_count * coarse_dev, share), F32),
            vmem((ranks - 1, q_share, tok), F32),
            dma((ranks,)), dma((ranks,)),
            pair(), pair(), pair(), pair(), pair(), pair(),
            dma((inner_count - 1,)), dma((inner_count - 1,)),
            dma((inner_count - 1,)), dma((inner_count - 1,)),
            dma((levels,)), dma((levels,)),
            dma((ranks - 1, heads // UNITS)), dma((ranks - 1, heads // UNITS)),
        ],
        compiler_params=pltpu.CompilerParams(
            collective_id=0, has_side_effects=True, vmem_limit_bytes=48 * 1024 * 1024),
    )(*(pltpu.with_memory_space_constraint(array, pltpu.HBM) for array in (
        queries, keys, values, pool_fine.T, pool_coarse)))
    return pl.pallas_call(
        norm_kernel,
        out_shape=jax.ShapeDtypeStruct((tok, HQ * HD), BF16),
        in_specs=[pl.BlockSpec(memory_space=pltpu.VMEM)] * 2,
        out_specs=pl.BlockSpec(memory_space=pltpu.VMEM),
        compiler_params=pltpu.CompilerParams(vmem_limit_bytes=8 * 1024 * 1024),
    )(attended, gain.reshape(1, -1))


def solution(mesh):
    rows = P(("outer", "inner"), None)
    return jax.shard_map(
        functools.partial(local, mesh.shape["outer"], mesh.shape["inner"]),
        mesh=mesh, in_specs=(rows, rows, rows, P(), P(), P()),
        out_specs=rows, check_vma=False,
    )
```

```python
import contextlib
import functools
import math

import jax
import jax.numpy as jnp
from jax import lax
from jax.experimental import pallas as pl
from jax.experimental.pallas import tpu as pltpu
from jax.sharding import PartitionSpec as P

HQ = 16
KVH = 4
HD = 64
BLOCK = 512
FINE = 16
RATIO = 8
COARSE = 128

EPSILON = 1e-06
LANES = 128
ONES = 16
UNITS = 4
MESH = pl.DeviceIdType.MESH
BF16 = jnp.bfloat16
F32 = jnp.float32
FACTOR = HD ** (-0.5) * math.log2(math.e)


def scope(name):
    return contextlib.nullcontext()


def kernel(
    outer_count, inner_count, use_fine,
    q_hbm, k_hbm, v_hbm, pf_hbm, pc_hbm, out_ref,
    q_ref, k_ref, v_ref, pf_ref, pc_ref, in_sems,
    q_all, queries_t, values_t, own_k, own_v, mate_k, mate_v, other_k, other_v,
    score_ref, weight_ref, peaks, sums, peak_now, decay_next, decay_now,
    fine_send, fine_all, coarse_send, coarse_pad, coarse_all,
    att_send,
    q_ss, q_rs, own_ss, own_rs, mate_ss, mate_rs, other_ss, other_rs,
    fine_ss, fine_rs, cg_ss, cg_rs, co_ss, co_rs, att_ss, att_rs,
):
    tok = q_ref.shape[0]
    ranks = BLOCK // tok
    kv_width = KVH * HD
    share = kv_width // ranks
    q_share = HQ * HD // ranks
    tiles = q_share // LANES
    heads = q_share // HD
    kv_local = share // HD
    heads_kv = heads // kv_local
    fine_dev = tok // FINE
    coarse_dev = tok // COARSE
    group_tok = tok * inner_count
    fine_amount = group_tok // FINE if use_fine else 0
    coarse_group = inner_count * coarse_dev
    coarse_amount = outer_count * coarse_group
    blocks = outer_count * inner_count // ranks
    levels = outer_count.bit_length() - 1

    o_me = lax.axis_index("outer")
    i_me = lax.axis_index("inner")
    linear = o_me * inner_count + i_me
    block = linear // ranks
    rank = lax.rem(linear, ranks)
    odd = lax.rem(block, 2)
    mate = block + 1 - 2 * odd
    relay_from = block - 2 + 4 * odd
    relay_to = block + 2 - 4 * odd
    has_other = (relay_from >= 0) & (relay_from < blocks)
    has_next = (relay_to >= 0) & (relay_to < blocks)

    def at_rank(which_block, rel):
        target_rank = lax.rem(rank + rel, ranks)
        spot = which_block * ranks + target_rank
        return (spot // inner_count, lax.rem(spot, inner_count)), target_rank

    inner_peers = [lax.rem(i_me + rel, inner_count) for rel in range(1, inner_count)]
    outer_peers = [
        o_me + 2 ** level * (1 - 2 * lax.rem(o_me // 2 ** level, 2)) for level in range(levels)]

    loads = [
        pltpu.make_async_copy(src, dst, in_sems.at[n])
        for n, (src, dst) in enumerate((
            (k_hbm, k_ref), (q_hbm, q_ref), (v_hbm, v_ref), (pf_hbm, pf_ref), (pc_hbm, pc_ref)))
    ]
    for load in loads:
        load.start()

    barrier = pltpu.get_barrier_semaphore()

    def greet(device):
        pl.semaphore_signal(barrier, inc=1, device_id=device, device_id_type=MESH)

    for peer in inner_peers:
        greet((o_me, peer))
    for peer in outer_peers:
        greet((peer, i_me))
    for which, there in ((relay_from, has_other), (relay_to, has_next)):
        @pl.when(there)
        def _():
            greet(at_rank(which, 0)[0])

    def remote(src, dst, send_sem, recv_sem, device):
        return pltpu.make_async_remote_copy(
            src_ref=src, dst_ref=dst, send_sem=send_sem, recv_sem=recv_sem,
            device_id=device, device_id_type=MESH,
        )

    def cols(index, width):
        return pl.ds(pl.multiple_of(index * width, LANES), width)

    def k_at(ref, slot):
        return ref.at[pl.ds(slot * tok, tok)]

    def v_at(ref, slot):
        return ref.at[:, pl.ds(0, HD), pl.ds(slot * tok, tok)]

    own_k_copies, own_q_copies, own_v_copies = [], [], []
    for rel in range(1, ranks):
        device, target = at_rank(block, rel)
        slot = ranks - rel
        own_k_copies.append(remote(
            k_ref.at[:, cols(target, share)], k_at(own_k, slot),
            own_ss.at[0, slot], own_rs.at[0, slot], device))
        own_q_copies.append(remote(
            q_ref.at[:, cols(target, q_share)], q_all.at[slot],
            q_ss.at[slot], q_rs.at[slot], device))
        own_v_copies.append(remote(
            values_t.at[target], v_at(own_v, slot),
            own_ss.at[1, slot], own_rs.at[1, slot], device))
    mate_k_copies, mate_v_copies = [], []
    for rel in range(ranks):
        device, target = at_rank(mate, rel)
        slot = (ranks - rel) % ranks
        mate_k_copies.append(remote(
            k_ref.at[:, cols(target, share)], k_at(mate_k, slot),
            mate_ss.at[0, slot], mate_rs.at[0, slot], device))
        mate_v_copies.append(remote(
            values_t.at[target], v_at(mate_v, slot),
            mate_ss.at[1, slot], mate_rs.at[1, slot], device))
    next_device = at_rank(relay_to, 0)[0]
    relay_k_copies = [remote(
        k_at(mate_k, slot), k_at(other_k, slot),
        other_ss.at[0, slot], other_rs.at[0, slot], next_device) for slot in range(ranks)]
    relay_v_copies = [remote(
        v_at(mate_v, slot), v_at(other_v, slot),
        other_ss.at[1, slot], other_rs.at[1, slot], next_device) for slot in range(ranks)]
    group_copies, fine_copies = [], []
    for n, peer in enumerate(inner_peers):
        peer_rank = lax.rem(peer, ranks)
        group_copies.append(remote(
            coarse_send.at[peer_rank], coarse_pad.at[i_me],
            cg_ss.at[n], cg_rs.at[n], (o_me, peer)))
        if use_fine:
            fine_copies.append(remote(
                fine_send.at[peer_rank], fine_all.at[i_me],
                fine_ss.at[n], fine_rs.at[n], (o_me, peer)))
    outer_copies = []
    for level, peer in enumerate(outer_peers):
        size = 2 ** level
        span = pl.ds(o_me // size * size, size)
        outer_copies.append(remote(
            coarse_all.at[span], coarse_all.at[span], co_ss.at[level], co_rs.at[level],
            (peer, i_me)))

    queries_t[...] = jnp.zeros(queries_t.shape, BF16)
    for ref in (own_v, mate_v, other_v):
        ref[:, HD:, :] = jnp.ones((kv_local, ONES, ref.shape[2]), BF16)

    with scope("wk"):
        loads[0].wait()
    with scope("wbar"):
        pl.semaphore_wait(
            barrier, inner_count - 1 + levels + has_other.astype(jnp.int32) + has_next.astype(jnp.int32))
    for copy in own_k_copies + mate_k_copies[:1]:
        copy.start()
    with scope("wq"):
        loads[1].wait()
    for copy in own_q_copies:
        copy.start()
    with scope("wv"):
        for load in loads[2:]:
            load.wait()

    def spread(pool):
        rows = pool.shape[0]
        return jnp.concatenate(
            [jnp.broadcast_to(pool[:, n:n + 1], (rows, HD)) for n in range(2 * KVH)], axis=1)

    pf = spread(pf_ref[...].T)
    pc = spread(pc_ref[...])
    paired = jnp.concatenate([k_ref[...], v_ref[...]], axis=1).astype(F32)
    fine = jnp.sum(paired.reshape(fine_dev, FINE, 2 * kv_width) * pf[None], axis=1).astype(BF16)
    fine_wide = fine.astype(F32)
    coarse_wide = jnp.sum(
        fine_wide.reshape(coarse_dev, RATIO, 2 * kv_width) * pc[None], axis=1
    ).astype(BF16).astype(F32)
    padded = coarse_send.shape[1]
    for n in range(ranks):
        k_cols = slice(n * share, (n + 1) * share)
        v_cols = slice(kv_width + n * share, kv_width + (n + 1) * share)
        if use_fine:
            fine_send[n] = jnp.concatenate([fine[:, k_cols], fine[:, v_cols]], axis=1)
        parts = [coarse_wide[:, k_cols], coarse_wide[:, v_cols]]
        if padded > 2 * coarse_dev:
            parts.append(jnp.zeros((padded - 2 * coarse_dev, share), F32))
        coarse_send[n] = jnp.concatenate(parts, axis=0)
    coarse_pad[i_me] = coarse_send[rank]
    if use_fine:
        fine_all[i_me] = fine_send[rank]
    for copy in group_copies + mate_k_copies[1:]:
        copy.start()
    turned = v_ref[...].T
    for n in range(ranks):
        for x in range(kv_local):
            row = n * share + x * HD
            values_t[n, x] = turned[row:row + HD]
    for copy in own_v_copies + mate_v_copies + fine_copies:
        copy.start()

    def arrange(part, tile_of):
        for x in range(tiles):
            turned = tile_of(x).T
            low = (2 * x // heads_kv) * HD
            for y in range(2):
                queries_t[part * heads + 2 * x + y, low:low + HD, :] = turned[y * HD:(y + 1) * HD]

    def score(unit, n, k_set, first):
        amount = k_set.shape[0]
        scores = jnp.dot(k_set, queries_t[unit], preferred_element_type=F32)
        peak = jnp.max(scores, axis=0, keepdims=True)
        if not first:
            before = peaks[unit]
            peak = jnp.maximum(peak, before)
            decay_next[n] = jnp.exp2((before - peak) * FACTOR)
        score_ref[n, 0:amount, :] = scores
        peaks[unit] = peak
        peak_now[n] = peak

    def weigh(n, amount, first):
        weight_ref[n, 0:amount, :] = jnp.exp2(
            (score_ref[n, 0:amount, :] - peak_now[n]) * FACTOR).astype(BF16)
        if not first:
            decay_now[n] = decay_next[n]

    def blend(unit, n, v_set, first):
        amount = v_set.shape[1]
        blended = jnp.dot(v_set, weight_ref[n, 0:amount, :], preferred_element_type=F32)
        sums[unit] = blended if first else sums[unit] * decay_now[n] + blended

    def run(groups, after):
        count = len(groups)
        for step in range(count + 2):
            if step >= 2:
                units, _, v_of, amount, first = groups[step - 2]
                for n, unit in enumerate(units):
                    blend(unit, n, v_of(unit % heads // heads_kv), first)
            if 1 <= step < count + 1:
                units, _, _, amount, first = groups[step - 1]
                for n in range(len(units)):
                    weigh(n, amount, first)
            if step < count:
                units, k_of, _, amount, first = groups[step]
                k_set = k_of()
                for n, unit in enumerate(units):
                    score(unit, n, k_set, first)
            if step - 2 in after:
                after[step - 2]()

    def units_of(part):
        base = part * heads
        return [list(range(base + n, base + n + UNITS)) for n in range(0, heads, UNITS)]

    def groups_of(parts, k_ref_, v_ref_, span, first):
        amount = span.stop - span.start
        return [
            (units, lambda: k_ref_[span, :], lambda g: v_ref_[g, :, span], amount, first)
            for part in parts for units in units_of(part)]

    def collect():
        with scope("w_group"):
            for copy in group_copies:
                copy.wait_recv()
        for n in range(inner_count):
            rows = slice(n * coarse_dev, (n + 1) * coarse_dev)
            lower = slice(coarse_group + n * coarse_dev, coarse_group + (n + 1) * coarse_dev)
            coarse_all[o_me, rows, :] = coarse_pad[n, 0:coarse_dev, :]
            coarse_all[o_me, lower, :] = coarse_pad[n, coarse_dev:2 * coarse_dev, :]

    def climb(level):
        if level > 0:
            outer_copies[level - 1].wait_recv()
        if level < levels:
            outer_copies[level].start()

    with scope("prep0"):
        own_k[0:tok, :] = k_ref[:, cols(rank, share)]
        own_v[:, 0:HD, 0:tok] = values_t[rank]
        arrange(0, lambda x: q_ref[:, cols(rank * tiles + x, LANES)])
    with scope("own0"):
        run(groups_of([0], own_k, own_v, slice(0, tok), True), {})

    with scope("w_own"):
        for copy in own_k_copies + own_q_copies + own_v_copies:
            copy.wait_recv()
    with scope("prep1"):
        for slot in range(1, ranks):
            arrange(slot, lambda x: q_all[slot, :, x * LANES:(x + 1) * LANES])
    with scope("own1"):
        run(groups_of(range(1, ranks), own_k, own_v, slice(0, BLOCK), True)
            + groups_of([0], own_k, own_v, slice(tok, BLOCK), False),
            {1: lambda: (collect(), climb(0))})

    with scope("w_mk"):
        for copy in mate_k_copies:
            copy.wait_recv()

    @pl.when(has_next)
    def _():
        for copy in relay_k_copies:
            copy.start()

    with scope("climb1"):
        climb(1)
    with scope("w_mv"):
        for copy in mate_v_copies:
            copy.wait_recv()

    @pl.when(has_next)
    def _():
        for copy in relay_v_copies:
            copy.start()

    with scope("mate"):
        run(groups_of(range(ranks), mate_k, mate_v, slice(0, BLOCK), False),
            {1: lambda: [climb(level) for level in range(2, levels)]})

    with scope("climb3"):
        climb(levels)
    with scope("far"):
        far = fine_amount + coarse_amount
        k_far = coarse_all[:, 0:coarse_group, :].reshape(coarse_amount, share)
        v_far = coarse_all[:, coarse_group:, :].reshape(coarse_amount, share)
        if use_fine:
            for copy in fine_copies:
                copy.wait_recv()
            fine_rows = fine_all[...].reshape(fine_amount, 2 * share).astype(F32)
            k_far = jnp.concatenate([fine_rows[:, :share], k_far], axis=0)
            v_far = jnp.concatenate([fine_rows[:, share:], v_far], axis=0)

        def reachable(shape, axis):
            spot = lax.broadcasted_iota(jnp.int32, shape, axis)
            fine_pos = o_me * group_tok + spot * FINE
            coarse_pos = (spot - fine_amount) * COARSE
            position = jnp.where(spot < fine_amount, fine_pos, coarse_pos)
            distance = jnp.abs(lax.div(position, BLOCK) - block)
            outside = (spot < fine_amount) | (lax.div(position, group_tok) != o_me)
            return (distance > 1) & outside

        stand_in = own_k[0:16, :].astype(F32)[0:1, :]
        other_k[BLOCK:, :] = jnp.where(
            reachable((far, share), 0), k_far, jnp.broadcast_to(stand_in, (far, share))).astype(BF16)
        open_cols = reachable((HD, far), 1)
        turned = v_far.T
        for x in range(kv_local):
            other_v[x, 0:HD, BLOCK:] = jnp.where(
                open_cols, turned[x * HD:(x + 1) * HD, :], 0.0).astype(BF16)
            other_v[x, HD:, BLOCK:] = open_cols[0:ONES].astype(F32).astype(BF16)

    @pl.when(has_other)
    def _():
        with scope("w_other"):
            for copy in relay_k_copies + relay_v_copies:
                copy.wait_recv()

    @pl.when(jnp.logical_not(has_other))
    def _():
        other_k[0:BLOCK, :] = own_k[...]
        other_v[:, :, 0:BLOCK] = jnp.zeros((kv_local, HD + ONES, BLOCK), BF16)

    def finish(unit):
        total = sums[unit]
        return total[0:HD] / total[HD:HD + 1]

    def att_copy(part, at):
        device, _ = at_rank(block, part)
        slot = ranks - part - 1
        row = pl.multiple_of(rank * q_share + at * UNITS * HD, HD)
        return remote(att_send.at[part - 1, pl.ds(at * UNITS * HD, UNITS * HD)],
                      out_ref.at[pl.ds(row, UNITS * HD)],
                      att_ss.at[slot, at], att_rs.at[slot, at], device)

    order = list(range(1, ranks)) + [0]
    per_part = heads // UNITS

    def after(index):
        part, at = order[index // per_part], index % per_part
        for n in range(UNITS):
            head = at * UNITS + n
            attended = finish(part * heads + head)
            if part:
                att_send[part - 1, head * HD:(head + 1) * HD, :] = attended
            else:
                out_ref[pl.ds(pl.multiple_of(rank * q_share + head * HD, HD), HD), :] = attended
        if part:
            att_copy(part, at).start()

    with scope("other"):
        run(groups_of(order, other_k, other_v, slice(0, BLOCK + far), False),
            {n: functools.partial(after, n) for n in range(ranks * per_part)})

    with scope("w_att"):
        for part in range(1, ranks):
            for at in range(per_part):
                att_copy(part, at).wait_recv()

    with scope("w_send"):
        for copy in (own_k_copies + own_q_copies + own_v_copies + mate_k_copies + mate_v_copies
                     + group_copies + fine_copies + outer_copies):
            copy.wait_send()

        @pl.when(has_next)
        def _():
            for copy in relay_k_copies + relay_v_copies:
                copy.wait_send()

        for part in range(1, ranks):
            for at in range(per_part):
                att_copy(part, at).wait_send()


def norm_kernel(attended_ref, gain_ref, out_ref):
    attended = attended_ref[...]
    rescale = lax.rsqrt(jnp.mean(attended * attended, axis=0, keepdims=True) + EPSILON)
    out_ref[...] = ((attended * rescale).T * gain_ref[...]).astype(BF16)


def local(outer_count, inner_count, queries, keys, values, pool_fine, pool_coarse, gain):
    tok = queries.shape[0]
    ranks = BLOCK // tok
    share = KVH * HD // ranks
    kv_local = share // HD
    q_share = HQ * HD // ranks
    heads = q_share // HD
    group_tok = tok * inner_count
    use_fine = group_tok > 2 * BLOCK
    far = (group_tok // FINE if use_fine else 0) + outer_count * group_tok // COARSE
    coarse_dev = tok // COARSE
    padded = -(-2 * coarse_dev // 8) * 8
    levels = outer_count.bit_length() - 1
    assert ranks >= 2 and BLOCK % tok == 0 and kv_local == 2 and share == LANES
    assert inner_count % (2 * ranks) == 0 and outer_count == 2 ** levels
    dma = pltpu.SemaphoreType.DMA
    vmem = pltpu.VMEM
    units = ranks * heads
    pair = lambda: dma((2, ranks))
    k_set = lambda amount: vmem((amount, share), BF16)
    v_set = lambda amount: vmem((kv_local, HD + ONES, amount), BF16)
    line = lambda: vmem((UNITS, 1, tok), F32)
    attended = pl.pallas_call(
        functools.partial(kernel, outer_count, inner_count, use_fine),
        out_shape=jax.ShapeDtypeStruct((HQ * HD, tok), F32),
        in_specs=[pl.BlockSpec(memory_space=pltpu.HBM)] * 5,
        out_specs=pl.BlockSpec(memory_space=pltpu.VMEM),
        scratch_shapes=[
            vmem(queries.shape, BF16), vmem(keys.shape, BF16), vmem(values.shape, BF16),
            vmem(pool_fine.shape[::-1], F32), vmem(pool_coarse.shape, F32), dma((5,)),
            vmem((ranks, tok, q_share), BF16),
            vmem((units, share, tok), BF16),
            vmem((ranks, kv_local, HD, tok), BF16),
            k_set(BLOCK), v_set(BLOCK), k_set(BLOCK), v_set(BLOCK),
            k_set(BLOCK + far), v_set(BLOCK + far),
            vmem((UNITS, BLOCK + far, tok), F32),
            vmem((UNITS, BLOCK + far, tok), BF16),
            vmem((units, 1, tok), F32),
            vmem((units, HD + ONES, tok), F32),
            line(), line(), line(),
            vmem((ranks, tok // FINE, 2 * share), BF16),
            vmem((inner_count, tok // FINE, 2 * share), BF16),
            vmem((ranks, padded, share), F32),
            vmem((inner_count, padded, share), F32),
            vmem((outer_count, 2 * inner_count * coarse_dev, share), F32),
            vmem((ranks - 1, q_share, tok), F32),
            dma((ranks,)), dma((ranks,)),
            pair(), pair(), pair(), pair(), pair(), pair(),
            dma((inner_count - 1,)), dma((inner_count - 1,)),
            dma((inner_count - 1,)), dma((inner_count - 1,)),
            dma((levels,)), dma((levels,)),
            dma((ranks - 1, heads // UNITS)), dma((ranks - 1, heads // UNITS)),
        ],
        compiler_params=pltpu.CompilerParams(
            collective_id=0, has_side_effects=True, vmem_limit_bytes=48 * 1024 * 1024),
    )(*(pltpu.with_memory_space_constraint(array, pltpu.HBM) for array in (
        queries, keys, values, pool_fine.T, pool_coarse)))
    return pl.pallas_call(
        norm_kernel,
        out_shape=jax.ShapeDtypeStruct((tok, HQ * HD), BF16),
        in_specs=[pl.BlockSpec(memory_space=pltpu.VMEM)] * 2,
        out_specs=pl.BlockSpec(memory_space=pltpu.VMEM),
        compiler_params=pltpu.CompilerParams(vmem_limit_bytes=8 * 1024 * 1024),
    )(attended, gain.reshape(1, -1))


def solution(mesh):
    rows = P(("outer", "inner"), None)
    return jax.shard_map(
        functools.partial(local, mesh.shape["outer"], mesh.shape["inner"]),
        mesh=mesh, in_specs=(rows, rows, rows, P(), P(), P()),
        out_specs=rows, check_vma=False,
    )
```

```python
import contextlib
import functools
import math

import jax
import jax.numpy as jnp
from jax import lax
from jax.experimental import pallas as pl
from jax.experimental.pallas import tpu as pltpu
from jax.sharding import PartitionSpec as P

HQ = 16
KVH = 4
HD = 64
BLOCK = 512
FINE = 16
RATIO = 8
COARSE = 128

EPSILON = 1e-06
LANES = 128
ONES = 16
UNITS = 4
MESH = pl.DeviceIdType.MESH
BF16 = jnp.bfloat16
F32 = jnp.float32
FACTOR = HD ** (-0.5) * math.log2(math.e)


def scope(name):
    return contextlib.nullcontext()


def kernel(
    outer_count, inner_count, use_fine,
    q_hbm, k_hbm, v_hbm, pf_hbm, pc_hbm, out_ref, got_ref,
    q_ref, k_ref, v_ref, pf_ref, pc_ref, in_sems,
    q_all, queries_t, values_t, own_k, own_v, mate_k, mate_v, other_k, other_v, far_k, far_v,
    score_ref, weight_ref, peaks, sums, peak_now, decay_next, decay_now,
    fine_send, fine_all, coarse_send, coarse_pad, coarse_all,
    att_send,
    q_ss, q_rs, own_ss, own_rs, mate_ss, mate_rs, other_ss, other_rs,
    fine_ss, fine_rs, cg_ss, cg_rs, co_ss, co_rs, att_ss, att_rs,
):
    tok = q_ref.shape[0]
    ranks = BLOCK // tok
    kv_width = KVH * HD
    share = kv_width // ranks
    q_share = HQ * HD // ranks
    tiles = q_share // LANES
    heads = q_share // HD
    kv_local = share // HD
    heads_kv = heads // kv_local
    fine_dev = tok // FINE
    coarse_dev = tok // COARSE
    group_tok = tok * inner_count
    fine_amount = group_tok // FINE if use_fine else 0
    coarse_group = inner_count * coarse_dev
    coarse_amount = outer_count * coarse_group
    blocks = outer_count * inner_count // ranks
    levels = outer_count.bit_length() - 1

    o_me = lax.axis_index("outer")
    i_me = lax.axis_index("inner")
    linear = o_me * inner_count + i_me
    block = linear // ranks
    rank = lax.rem(linear, ranks)
    odd = lax.rem(block, 2)
    mate = block + 1 - 2 * odd
    relay_from = block - 2 + 4 * odd
    relay_to = block + 2 - 4 * odd
    has_other = (relay_from >= 0) & (relay_from < blocks)
    has_next = (relay_to >= 0) & (relay_to < blocks)

    def at_rank(which_block, rel):
        target_rank = lax.rem(rank + rel, ranks)
        spot = which_block * ranks + target_rank
        return (spot // inner_count, lax.rem(spot, inner_count)), target_rank

    inner_peers = [lax.rem(i_me + rel, inner_count) for rel in range(1, inner_count)]
    outer_peers = [
        o_me + 2 ** level * (1 - 2 * lax.rem(o_me // 2 ** level, 2)) for level in range(levels)]

    loads = [
        pltpu.make_async_copy(src, dst, in_sems.at[n])
        for n, (src, dst) in enumerate((
            (k_hbm, k_ref), (q_hbm, q_ref), (v_hbm, v_ref), (pf_hbm, pf_ref), (pc_hbm, pc_ref)))
    ]
    for load in loads:
        load.start()

    barrier = pltpu.get_barrier_semaphore()

    def greet(device):
        pl.semaphore_signal(barrier, inc=1, device_id=device, device_id_type=MESH)

    for peer in inner_peers:
        greet((o_me, peer))
    for peer in outer_peers:
        greet((peer, i_me))
    for which, there in ((relay_from, has_other), (relay_to, has_next)):
        @pl.when(there)
        def _():
            greet(at_rank(which, 0)[0])

    def remote(src, dst, send_sem, recv_sem, device):
        return pltpu.make_async_remote_copy(
            src_ref=src, dst_ref=dst, send_sem=send_sem, recv_sem=recv_sem,
            device_id=device, device_id_type=MESH,
        )

    def cols(index, width):
        return pl.ds(pl.multiple_of(index * width, LANES), width)

    def k_at(ref, slot):
        return ref.at[pl.ds(slot * tok, tok)]

    def v_at(ref, slot):
        return ref.at[:, pl.ds(0, HD), pl.ds(slot * tok, tok)]

    own_k_copies, own_q_copies, own_v_copies = [], [], []
    for rel in range(1, ranks):
        device, target = at_rank(block, rel)
        slot = ranks - rel
        own_k_copies.append(remote(
            k_ref.at[:, cols(target, share)], k_at(own_k, slot),
            own_ss.at[0, slot], own_rs.at[0, slot], device))
        own_q_copies.append(remote(
            q_ref.at[:, cols(target, q_share)], q_all.at[slot],
            q_ss.at[slot], q_rs.at[slot], device))
        own_v_copies.append(remote(
            values_t.at[target], v_at(own_v, slot),
            own_ss.at[1, slot], own_rs.at[1, slot], device))
    mate_k_copies, mate_v_copies = [], []
    for rel in range(ranks):
        device, target = at_rank(mate, rel)
        slot = (ranks - rel) % ranks
        mate_k_copies.append(remote(
            k_ref.at[:, cols(target, share)], k_at(mate_k, slot),
            mate_ss.at[0, slot], mate_rs.at[0, slot], device))
        mate_v_copies.append(remote(
            values_t.at[target], v_at(mate_v, slot),
            mate_ss.at[1, slot], mate_rs.at[1, slot], device))
    next_device = at_rank(relay_to, 0)[0]
    relay_k_copies = [remote(
        k_at(mate_k, slot), k_at(other_k, slot),
        other_ss.at[0, slot], other_rs.at[0, slot], next_device) for slot in range(ranks)]
    relay_v_copies = [remote(
        v_at(mate_v, slot), v_at(other_v, slot),
        other_ss.at[1, slot], other_rs.at[1, slot], next_device) for slot in range(ranks)]
    group_copies, fine_copies = [], []
    for n, peer in enumerate(inner_peers):
        peer_rank = lax.rem(peer, ranks)
        group_copies.append(remote(
            coarse_send.at[peer_rank], coarse_pad.at[i_me],
            cg_ss.at[n], cg_rs.at[n], (o_me, peer)))
        if use_fine:
            fine_copies.append(remote(
                fine_send.at[peer_rank], fine_all.at[i_me],
                fine_ss.at[n], fine_rs.at[n], (o_me, peer)))
    outer_copies = []
    for level, peer in enumerate(outer_peers):
        size = 2 ** level
        span = pl.ds(o_me // size * size, size)
        outer_copies.append(remote(
            coarse_all.at[span], coarse_all.at[span], co_ss.at[level], co_rs.at[level],
            (peer, i_me)))

    queries_t[...] = jnp.zeros(queries_t.shape, BF16)
    for ref in (own_v, mate_v, other_v):
        ref[:, HD:, :] = jnp.ones((kv_local, ONES, ref.shape[2]), BF16)

    with scope("wload"):
        for load in loads:
            load.wait()

    def spread(pool):
        rows = pool.shape[0]
        return jnp.concatenate(
            [jnp.broadcast_to(pool[:, n:n + 1], (rows, HD)) for n in range(2 * KVH)], axis=1)

    pf = spread(pf_ref[...].T)
    pc = spread(pc_ref[...])
    paired = jnp.concatenate([k_ref[...], v_ref[...]], axis=1).astype(F32)
    fine = jnp.sum(paired.reshape(fine_dev, FINE, 2 * kv_width) * pf[None], axis=1).astype(BF16)
    fine_wide = fine.astype(F32)
    coarse_wide = jnp.sum(
        fine_wide.reshape(coarse_dev, RATIO, 2 * kv_width) * pc[None], axis=1
    ).astype(BF16).astype(F32)
    padded = coarse_send.shape[1]
    for n in range(ranks):
        k_cols = slice(n * share, (n + 1) * share)
        v_cols = slice(kv_width + n * share, kv_width + (n + 1) * share)
        if use_fine:
            fine_send[n] = jnp.concatenate([fine[:, k_cols], fine[:, v_cols]], axis=1)
        parts = [coarse_wide[:, k_cols], coarse_wide[:, v_cols]]
        if padded > 2 * coarse_dev:
            parts.append(jnp.zeros((padded - 2 * coarse_dev, share), F32))
        coarse_send[n] = jnp.concatenate(parts, axis=0)
    coarse_pad[i_me] = coarse_send[rank]
    if use_fine:
        fine_all[i_me] = fine_send[rank]
    turned = v_ref[...].T
    for n in range(ranks):
        for x in range(kv_local):
            row = n * share + x * HD
            values_t[n, x] = turned[row:row + HD]
    with scope("wbar"):
        pl.semaphore_wait(
            barrier, inner_count - 1 + levels + has_other.astype(jnp.int32) + has_next.astype(jnp.int32))
    for copy in group_copies + own_k_copies + mate_k_copies[:1] + own_q_copies + own_v_copies:
        copy.start()

    def arrange(part, tile_of):
        for x in range(tiles):
            turned = tile_of(x).T
            low = (2 * x // heads_kv) * HD
            for y in range(2):
                queries_t[part * heads + 2 * x + y, low:low + HD, :] = turned[y * HD:(y + 1) * HD]

    def score(unit, n, k_set, first):
        amount = k_set.shape[0]
        scores = jnp.dot(k_set, queries_t[unit], preferred_element_type=F32)
        peak = jnp.max(scores, axis=0, keepdims=True)
        if not first:
            before = peaks[unit]
            peak = jnp.maximum(peak, before)
            decay_next[n] = jnp.exp2((before - peak) * FACTOR)
        score_ref[n, 0:amount, :] = scores
        peaks[unit] = peak
        peak_now[n] = peak

    def weigh(unit, n, amount, first):
        weight_ref[unit, 0:amount, :] = jnp.exp2(
            (score_ref[n, 0:amount, :] - peak_now[n]) * FACTOR).astype(BF16)
        if not first:
            decay_now[unit] = decay_next[n]

    def blend(unit, v_set, first):
        amount = v_set.shape[1]
        blended = jnp.dot(v_set, weight_ref[unit, 0:amount, :], preferred_element_type=F32)
        sums[unit] = blended if first else sums[unit] * decay_now[unit] + blended

    def run(groups, lag, hooks):
        count = len(groups)
        for step in range(count + lag):
            if step >= lag:
                units, _, v_of, amount, first = groups[step - lag]
                for unit in units:
                    blend(unit, v_of(unit % heads // heads_kv), first)
            if 1 <= step < count + 1:
                units, _, _, amount, first = groups[step - 1]
                for n, unit in enumerate(units):
                    weigh(unit, n, amount, first)
            if step < count:
                units, k_of, _, amount, first = groups[step]
                k_set = k_of()
                for n, unit in enumerate(units):
                    score(unit, n, k_set, first)
            if step in hooks:
                hooks[step]()

    def units_of(part):
        base = part * heads
        return [list(range(base + n, base + n + UNITS)) for n in range(0, heads, UNITS)]

    def groups_of(parts, k_ref_, v_ref_, span, first):
        amount = span.stop - span.start
        return [
            (units, lambda: k_ref_[span, :], lambda g: v_ref_[g, :, span], amount, first)
            for part in parts for units in units_of(part)]

    def collect():
        with scope("w_group"):
            for copy in group_copies:
                copy.wait_recv()
        for n in range(inner_count):
            rows = slice(n * coarse_dev, (n + 1) * coarse_dev)
            lower = slice(coarse_group + n * coarse_dev, coarse_group + (n + 1) * coarse_dev)
            coarse_all[o_me, rows, :] = coarse_pad[n, 0:coarse_dev, :]
            coarse_all[o_me, lower, :] = coarse_pad[n, coarse_dev:2 * coarse_dev, :]

    def climb(level):
        if level > 0:
            outer_copies[level - 1].wait_recv()
        if level < levels:
            outer_copies[level].start()

    with scope("prep0"):
        own_k[0:tok, :] = k_ref[:, cols(rank, share)]
        own_v[:, 0:HD, 0:tok] = values_t[rank]
        arrange(0, lambda x: q_ref[:, cols(rank * tiles + x, LANES)])
    with scope("own0"):
        run(groups_of([0], own_k, own_v, slice(0, tok), True), 2, {})
    for copy in mate_k_copies[1:]:
        copy.start()

    with scope("w_own"):
        for copy in own_k_copies + own_q_copies + own_v_copies:
            copy.wait_recv()
    for copy in mate_v_copies[:1]:
        copy.start()
    with scope("prep1"):
        for slot in range(1, ranks):
            arrange(slot, lambda x: q_all[slot, :, x * LANES:(x + 1) * LANES])

    def start_all(copies):
        for copy in copies:
            copy.start()

    def relay(name, arrivals, onward):
        with scope(name):
            for copy in arrivals:
                copy.wait_recv()

        @pl.when(has_next)
        def _():
            start_all(onward)

    with scope("own1"):
        run(groups_of(range(1, ranks), own_k, own_v, slice(0, BLOCK), True)
            + groups_of([0], own_k, own_v, slice(tok, BLOCK), False), 2,
            {0: lambda: start_all(mate_v_copies[1:] + fine_copies),
             2: lambda: (collect(), climb(0)),
             4: lambda: relay("w_mk0", mate_k_copies[:1], relay_k_copies[:1])})

    relay("w_mk1", mate_k_copies[1:], relay_k_copies[1:])
    with scope("climb1"):
        climb(1)
    mate_groups = groups_of(range(ranks), mate_k, mate_v, slice(0, BLOCK), False)
    with scope("mate"):
        run(mate_groups, len(mate_groups) + 1, {
            1: lambda: relay("w_mv0", mate_v_copies[:1], relay_v_copies[:1]),
            len(mate_groups): lambda: relay("w_mv1", mate_v_copies[1:], relay_v_copies[1:])})
    with scope("climb2"):
        for level in range(2, levels):
            climb(level)

    @pl.when(has_other)
    def _():
        with scope("w_other"):
            for copy in relay_k_copies:
                copy.wait_recv()

        def arrive():
            with scope("w_otherv"):
                for copy in relay_v_copies:
                    copy.wait_recv()

        other_groups = groups_of(range(ranks), other_k, other_v, slice(0, BLOCK), False)
        count = len(other_groups)
        with scope("other"):
            run(other_groups, count + 1, {count: arrive})

    with scope("climb3"):
        climb(levels)
    with scope("far"):
        far = fine_amount + coarse_amount
        k_far = coarse_all[:, 0:coarse_group, :].reshape(coarse_amount, share)
        v_far = coarse_all[:, coarse_group:, :].reshape(coarse_amount, share)
        if use_fine:
            for copy in fine_copies:
                copy.wait_recv()
            fine_rows = fine_all[...].reshape(fine_amount, 2 * share).astype(F32)
            k_far = jnp.concatenate([fine_rows[:, :share], k_far], axis=0)
            v_far = jnp.concatenate([fine_rows[:, share:], v_far], axis=0)

        def reachable(shape, axis):
            spot = lax.broadcasted_iota(jnp.int32, shape, axis)
            fine_pos = o_me * group_tok + spot * FINE
            coarse_pos = (spot - fine_amount) * COARSE
            position = jnp.where(spot < fine_amount, fine_pos, coarse_pos)
            distance = jnp.abs(lax.div(position, BLOCK) - block)
            outside = (spot < fine_amount) | (lax.div(position, group_tok) != o_me)
            return (distance > 1) & outside

        stand_in = own_k[0:16, :].astype(F32)[0:1, :]
        far_k[...] = jnp.where(
            reachable((far, share), 0), k_far, jnp.broadcast_to(stand_in, (far, share))).astype(BF16)
        open_cols = reachable((HD, far), 1)
        turned = v_far.T
        for x in range(kv_local):
            far_v[x, 0:HD, :] = jnp.where(
                open_cols, turned[x * HD:(x + 1) * HD, :], 0.0).astype(BF16)
            far_v[x, HD:, :] = open_cols[0:ONES].astype(F32).astype(BF16)

    def finish(unit):
        total = sums[unit]
        return total[0:HD] / total[HD:HD + 1]

    def att_copy(part, at):
        device, _ = at_rank(block, part)
        slot = ranks - part - 1
        span = pl.ds(at * UNITS * HD, UNITS * HD)
        return remote(att_send.at[part - 1, span], got_ref.at[slot, span],
                      att_ss.at[slot, at], att_rs.at[slot, at], device)

    order = list(range(1, ranks)) + [0]
    per_part = heads // UNITS

    def after(index):
        part, at = order[index // per_part], index % per_part
        for n in range(UNITS):
            head = at * UNITS + n
            attended = finish(part * heads + head)
            if part:
                att_send[part - 1, head * HD:(head + 1) * HD, :] = attended.astype(BF16)
            else:
                out_ref[head * HD:(head + 1) * HD, :] = attended
        if part:
            att_copy(part, at).start()

    far_groups = groups_of(order, far_k, far_v, slice(0, far), False)
    with scope("farrun"):
        run(far_groups, 2, {2 + n: functools.partial(after, n) for n in range(len(far_groups))})

    with scope("w_att"):
        for part in range(1, ranks):
            for at in range(per_part):
                att_copy(part, at).wait_recv()

    with scope("w_send"):
        for copy in (own_k_copies + own_q_copies + own_v_copies + mate_k_copies + mate_v_copies
                     + group_copies + fine_copies + outer_copies):
            copy.wait_send()

        @pl.when(has_next)
        def _():
            for copy in relay_k_copies + relay_v_copies:
                copy.wait_send()

        for part in range(1, ranks):
            for at in range(per_part):
                att_copy(part, at).wait_send()


def norm_kernel(kept_ref, got_ref, gain_ref, out_ref):
    parts = got_ref.shape[0] + 1
    width = kept_ref.shape[0]
    rank = lax.rem(lax.axis_index("inner"), parts)
    blocks = [kept_ref[...]] + [got_ref[n].astype(F32) for n in range(parts - 1)]
    total = sum(jnp.sum(x * x, axis=0, keepdims=True) for x in blocks)
    rescale = lax.rsqrt(total / (parts * width) + EPSILON)
    for n, x in enumerate(blocks):
        column = lax.rem(rank + n, parts)
        cols = pl.ds(pl.multiple_of(column * width, LANES), width)
        out_ref[:, cols] = ((x * rescale).T * gain_ref[:, cols]).astype(BF16)


def local(outer_count, inner_count, queries, keys, values, pool_fine, pool_coarse, gain):
    tok = queries.shape[0]
    ranks = BLOCK // tok
    share = KVH * HD // ranks
    kv_local = share // HD
    q_share = HQ * HD // ranks
    heads = q_share // HD
    group_tok = tok * inner_count
    use_fine = group_tok > 2 * BLOCK
    far = (group_tok // FINE if use_fine else 0) + outer_count * group_tok // COARSE
    coarse_dev = tok // COARSE
    padded = -(-2 * coarse_dev // 8) * 8
    levels = outer_count.bit_length() - 1
    assert ranks >= 2 and BLOCK % tok == 0 and kv_local == 2 and share == LANES
    assert inner_count % (2 * ranks) == 0 and outer_count == 2 ** levels
    dma = pltpu.SemaphoreType.DMA
    vmem = pltpu.VMEM
    units = ranks * heads
    pair = lambda: dma((2, ranks))
    k_set = lambda amount: vmem((amount, share), BF16)
    v_set = lambda amount: vmem((kv_local, HD + ONES, amount), BF16)
    line = lambda: vmem((UNITS, 1, tok), F32)
    kept, got = pl.pallas_call(
        functools.partial(kernel, outer_count, inner_count, use_fine),
        out_shape=[jax.ShapeDtypeStruct((q_share, tok), F32),
                   jax.ShapeDtypeStruct((ranks - 1, q_share, tok), BF16)],
        in_specs=[pl.BlockSpec(memory_space=pltpu.HBM)] * 5,
        out_specs=[pl.BlockSpec(memory_space=pltpu.VMEM)] * 2,
        scratch_shapes=[
            vmem(queries.shape, BF16), vmem(keys.shape, BF16), vmem(values.shape, BF16),
            vmem(pool_fine.shape[::-1], F32), vmem(pool_coarse.shape, F32), dma((5,)),
            vmem((ranks, tok, q_share), BF16),
            vmem((units, share, tok), BF16),
            vmem((ranks, kv_local, HD, tok), BF16),
            k_set(BLOCK), v_set(BLOCK), k_set(BLOCK), v_set(BLOCK),
            k_set(BLOCK), v_set(BLOCK), k_set(far), v_set(far),
            vmem((UNITS, max(BLOCK, far), tok), F32),
            vmem((units, max(BLOCK, far), tok), BF16),
            vmem((units, 1, tok), F32),
            vmem((units, HD + ONES, tok), F32),
            line(), line(), vmem((units, 1, tok), F32),
            vmem((ranks, tok // FINE, 2 * share), BF16),
            vmem((inner_count, tok // FINE, 2 * share), BF16),
            vmem((ranks, padded, share), F32),
            vmem((inner_count, padded, share), F32),
            vmem((outer_count, 2 * inner_count * coarse_dev, share), F32),
            vmem((ranks - 1, q_share, tok), BF16),
            dma((ranks,)), dma((ranks,)),
            pair(), pair(), pair(), pair(), pair(), pair(),
            dma((inner_count - 1,)), dma((inner_count - 1,)),
            dma((inner_count - 1,)), dma((inner_count - 1,)),
            dma((levels,)), dma((levels,)),
            dma((ranks - 1, heads // UNITS)), dma((ranks - 1, heads // UNITS)),
        ],
        compiler_params=pltpu.CompilerParams(
            collective_id=0, has_side_effects=True, vmem_limit_bytes=48 * 1024 * 1024),
    )(*(pltpu.with_memory_space_constraint(array, pltpu.HBM) for array in (
        queries, keys, values, pool_fine.T, pool_coarse)))
    return pl.pallas_call(
        norm_kernel,
        out_shape=jax.ShapeDtypeStruct((tok, HQ * HD), BF16),
        in_specs=[pl.BlockSpec(memory_space=pltpu.VMEM)] * 3,
        out_specs=pl.BlockSpec(memory_space=pltpu.VMEM),
        compiler_params=pltpu.CompilerParams(vmem_limit_bytes=8 * 1024 * 1024),
    )(kept, got, gain.reshape(1, -1))


def solution(mesh):
    rows = P(("outer", "inner"), None)
    return jax.shard_map(
        functools.partial(local, mesh.shape["outer"], mesh.shape["inner"]),
        mesh=mesh, in_specs=(rows, rows, rows, P(), P(), P()),
        out_specs=rows, check_vma=False,
    )
```

```python
import contextlib
import functools
import math

import jax
import jax.numpy as jnp
from jax import lax
from jax.experimental import pallas as pl
from jax.experimental.pallas import tpu as pltpu
from jax.sharding import PartitionSpec as P

HQ = 16
KVH = 4
HD = 64
BLOCK = 512
FINE = 16
RATIO = 8
COARSE = 128

EPSILON = 1e-06
LANES = 128
ONES = 16
UNITS = 4
MESH = pl.DeviceIdType.MESH
BF16 = jnp.bfloat16
F32 = jnp.float32
FACTOR = HD ** (-0.5) * math.log2(math.e)


def scope(name):
    return contextlib.nullcontext()


def kernel(
    outer_count, inner_count, use_fine,
    q_hbm, k_hbm, v_hbm, pf_hbm, pc_hbm, out_ref, got_ref,
    q_ref, k_ref, v_ref, pf_ref, pc_ref, in_sems,
    q_all, queries_t, values_t, own_k, own_v, mate_k, mate_v, other_k, other_v, far_k, far_v,
    score_ref, weight_ref, peaks, sums, peak_now, decay_next, decay_now, far_weights, far_decays,
    fine_send, fine_all, coarse_send, coarse_pad, coarse_all,
    att_send,
    q_ss, q_rs, own_ss, own_rs, mate_ss, mate_rs, other_ss, other_rs,
    fine_ss, fine_rs, cg_ss, cg_rs, co_ss, co_rs, att_ss, att_rs, token_sems,
):
    tok = q_ref.shape[0]
    ranks = BLOCK // tok
    kv_width = KVH * HD
    share = kv_width // ranks
    q_share = HQ * HD // ranks
    tiles = q_share // LANES
    heads = q_share // HD
    kv_local = share // HD
    heads_kv = heads // kv_local
    fine_dev = tok // FINE
    coarse_dev = tok // COARSE
    group_tok = tok * inner_count
    fine_amount = group_tok // FINE if use_fine else 0
    coarse_group = inner_count * coarse_dev
    coarse_amount = outer_count * coarse_group
    blocks = outer_count * inner_count // ranks
    turns = outer_count // 2 - 1

    o_me = lax.axis_index("outer")
    i_me = lax.axis_index("inner")
    linear = o_me * inner_count + i_me
    block = linear // ranks
    rank = lax.rem(linear, ranks)
    odd = lax.rem(block, 2)
    mate = block + 1 - 2 * odd
    relay_from = block - 2 + 4 * odd
    relay_to = block + 2 - 4 * odd
    has_other = (relay_from >= 0) & (relay_from < blocks)
    has_next = (relay_to >= 0) & (relay_to < blocks)

    def at_rank(which_block, rel):
        target_rank = lax.rem(rank + rel, ranks)
        spot = which_block * ranks + target_rank
        return (spot // inner_count, lax.rem(spot, inner_count)), target_rank

    inner_peers = [lax.rem(i_me + rel, inner_count) for rel in range(1, inner_count)]
    outer_peers = [lax.rem(o_me + rel, outer_count) for rel in range(1, outer_count)]

    loads = [
        pltpu.make_async_copy(src, dst, in_sems.at[n])
        for n, (src, dst) in enumerate((
            (k_hbm, k_ref), (q_hbm, q_ref), (v_hbm, v_ref), (pf_hbm, pf_ref), (pc_hbm, pc_ref)))
    ]
    for load in loads:
        load.start()

    barrier = pltpu.get_barrier_semaphore()

    def greet(device):
        pl.semaphore_signal(barrier, inc=1, device_id=device, device_id_type=MESH)

    for peer in inner_peers:
        greet((o_me, peer))
    greet((o_me + 1 - 2 * lax.rem(o_me, 2), i_me))
    line = ((o_me - 2, o_me >= 2), (o_me + 2, o_me + 2 < outer_count))
    near = [((o, i_me), there) for o, there in line]
    near += [(at_rank(which, 0)[0], there)
             for which, there in ((relay_from, has_other), (relay_to, has_next))]
    for device, there in near:
        @pl.when(there)
        def _():
            greet(device)
    line_count = sum(there.astype(jnp.int32) for _, there in line)
    near_count = sum(there.astype(jnp.int32) for _, there in near)

    def remote(src, dst, send_sem, recv_sem, device):
        return pltpu.make_async_remote_copy(
            src_ref=src, dst_ref=dst, send_sem=send_sem, recv_sem=recv_sem,
            device_id=device, device_id_type=MESH,
        )

    def cols(index, width):
        return pl.ds(pl.multiple_of(index * width, LANES), width)

    def k_at(ref, slot):
        return ref.at[pl.ds(slot * tok, tok)]

    def v_at(ref, slot):
        return ref.at[:, pl.ds(0, HD), pl.ds(slot * tok, tok)]

    own_k_copies, own_q_copies, own_v_copies = [], [], []
    for rel in range(1, ranks):
        device, target = at_rank(block, rel)
        slot = ranks - rel
        own_k_copies.append(remote(
            k_ref.at[:, cols(target, share)], k_at(own_k, slot),
            own_ss.at[0, slot], own_rs.at[0, slot], device))
        own_q_copies.append(remote(
            q_ref.at[:, cols(target, q_share)], q_all.at[slot],
            q_ss.at[slot], q_rs.at[slot], device))
        own_v_copies.append(remote(
            values_t.at[target], v_at(own_v, slot),
            own_ss.at[1, slot], own_rs.at[1, slot], device))
    mate_k_copies, mate_v_copies = [], []
    for rel in range(ranks):
        device, target = at_rank(mate, rel)
        slot = (ranks - rel) % ranks
        mate_k_copies.append(remote(
            k_ref.at[:, cols(target, share)], k_at(mate_k, slot),
            mate_ss.at[0, slot], mate_rs.at[0, slot], device))
        mate_v_copies.append(remote(
            values_t.at[target], v_at(mate_v, slot),
            mate_ss.at[1, slot], mate_rs.at[1, slot], device))
    next_device = at_rank(relay_to, 0)[0]
    relay_k_copies = [remote(
        k_at(mate_k, slot), k_at(other_k, slot),
        other_ss.at[0, slot], other_rs.at[0, slot], next_device) for slot in range(ranks)]
    relay_v_copies = [remote(
        v_at(mate_v, slot), v_at(other_v, slot),
        other_ss.at[1, slot], other_rs.at[1, slot], next_device) for slot in range(ranks)]
    group_copies, fine_copies = [], []
    for n, peer in enumerate(inner_peers):
        peer_rank = lax.rem(peer, ranks)
        group_copies.append(remote(
            coarse_send.at[peer_rank], coarse_pad.at[i_me],
            cg_ss.at[n], cg_rs.at[n], (o_me, peer)))
        if use_fine:
            fine_copies.append(remote(
                fine_send.at[peer_rank], fine_all.at[i_me],
                fine_ss.at[n], fine_rs.at[n], (o_me, peer)))
    outer_copies = [remote(
        coarse_all.at[o_me], coarse_all.at[o_me], co_ss.at[n], co_rs.at[n], (peer, i_me))
        for n, peer in enumerate(outer_peers)]

    queries_t[...] = jnp.zeros(queries_t.shape, BF16)
    for ref in (own_v, mate_v, other_v):
        ref[:, HD:, :] = jnp.ones((kv_local, ONES, ref.shape[2]), BF16)

    with scope("wload"):
        for load in loads:
            load.wait()

    def spread(pool):
        rows = pool.shape[0]
        return jnp.concatenate(
            [jnp.broadcast_to(pool[:, n:n + 1], (rows, HD)) for n in range(2 * KVH)], axis=1)

    pf = spread(pf_ref[...].T)
    pc = spread(pc_ref[...])
    paired = jnp.concatenate([k_ref[...], v_ref[...]], axis=1).astype(F32)
    fine = jnp.sum(paired.reshape(fine_dev, FINE, 2 * kv_width) * pf[None], axis=1).astype(BF16)
    fine_wide = fine.astype(F32)
    coarse_wide = jnp.sum(
        fine_wide.reshape(coarse_dev, RATIO, 2 * kv_width) * pc[None], axis=1
    ).astype(BF16).astype(F32)
    padded = coarse_send.shape[1]
    for n in range(ranks):
        k_cols = slice(n * share, (n + 1) * share)
        v_cols = slice(kv_width + n * share, kv_width + (n + 1) * share)
        if use_fine:
            fine_send[n] = jnp.concatenate([fine[:, k_cols], fine[:, v_cols]], axis=1)
        parts = [coarse_wide[:, k_cols], coarse_wide[:, v_cols]]
        if padded > 2 * coarse_dev:
            parts.append(jnp.zeros((padded - 2 * coarse_dev, share), F32))
        coarse_send[n] = jnp.concatenate(parts, axis=0)
    coarse_pad[i_me] = coarse_send[rank]
    if use_fine:
        fine_all[i_me] = fine_send[rank]
    turned = v_ref[...].T
    for n in range(ranks):
        for x in range(kv_local):
            row = n * share + x * HD
            values_t[n, x] = turned[row:row + HD]
    with scope("wbar"):
        pl.semaphore_wait(
            barrier, inner_count + near_count)

    def pass_on(turn):
        for o, there in line:
            @pl.when(there)
            def _():
                pl.semaphore_signal(
                    token_sems.at[turn], inc=1, device_id=(o, i_me), device_id_type=MESH)

    def hear(turn):
        if turn < turns:
            with scope("tok%d" % turn):
                pl.semaphore_wait(token_sems.at[turn], line_count)
        if turn + 1 < turns:
            pass_on(turn + 1)

    for copy in group_copies:
        copy.start()
    own_copies = own_k_copies + own_q_copies + own_v_copies

    @pl.when(rank == 0)
    def _():
        for copy in own_copies + mate_k_copies[:1]:
            copy.start()

    @pl.when(rank > 0)
    def _():
        for copy in mate_k_copies[:1] + own_copies:
            copy.start()

    if turns > 0:
        pass_on(0)

    def arrange(part, tile_of):
        for x in range(tiles):
            turned = tile_of(x).T
            low = (2 * x // heads_kv) * HD
            for y in range(2):
                queries_t[part * heads + 2 * x + y, low:low + HD, :] = turned[y * HD:(y + 1) * HD]

    def score(unit, n, k_set, first):
        amount = k_set.shape[0]
        scores = jnp.dot(k_set, queries_t[unit], preferred_element_type=F32)
        peak = jnp.max(scores, axis=0, keepdims=True)
        if not first:
            before = peaks[unit]
            peak = jnp.maximum(peak, before)
            decay_next[n] = jnp.exp2((before - peak) * FACTOR)
        score_ref[n, 0:amount, :] = scores
        peaks[unit] = peak
        peak_now[n] = peak

    def weigh(unit, n, amount, first, weights=weight_ref, decays=decay_now):
        weights[unit, 0:amount, :] = jnp.exp2(
            (score_ref[n, 0:amount, :] - peak_now[n]) * FACTOR).astype(BF16)
        if not first:
            decays[unit] = decay_next[n]

    def product(unit, v_set, weights):
        return jnp.dot(
            v_set, weights[unit, 0:v_set.shape[1], :], preferred_element_type=F32)

    def blend(unit, v_set, first):
        blended = product(unit, v_set, weight_ref)
        sums[unit] = blended if first else sums[unit] * decay_now[unit] + blended

    def run(groups, lag, hooks, *into):
        count = len(groups)
        for step in range(count + (1 if lag is None else lag)):
            if lag is not None and step >= lag:
                units, _, v_of, amount, first = groups[step - lag]
                for unit in units:
                    blend(unit, v_of(unit % heads // heads_kv), first)
            if 1 <= step < count + 1:
                units, _, _, amount, first = groups[step - 1]
                for n, unit in enumerate(units):
                    weigh(unit, n, amount, first, *into)
            if step < count:
                units, k_of, _, amount, first = groups[step]
                k_set = k_of()
                for n, unit in enumerate(units):
                    score(unit, n, k_set, first)
            if step in hooks:
                hooks[step]()

    def units_of(part):
        base = part * heads
        return [list(range(base + n, base + n + UNITS)) for n in range(0, heads, UNITS)]

    def groups_of(parts, k_ref_, v_ref_, span, first):
        amount = span.stop - span.start
        return [
            (units, lambda: k_ref_[span, :], lambda g: v_ref_[g, :, span], amount, first)
            for part in parts for units in units_of(part)]

    def collect():
        with scope("w_group"):
            for copy in group_copies:
                copy.wait_recv()
        for n in range(inner_count):
            rows = slice(n * coarse_dev, (n + 1) * coarse_dev)
            lower = slice(coarse_group + n * coarse_dev, coarse_group + (n + 1) * coarse_dev)
            coarse_all[o_me, rows, :] = coarse_pad[n, 0:coarse_dev, :]
            coarse_all[o_me, lower, :] = coarse_pad[n, coarse_dev:2 * coarse_dev, :]

    def share_coarse():
        collect()
        for turn in range(2, turns):
            hear(turn)
        start_all(outer_copies)

    def start_all(copies):
        for copy in copies:
            copy.start()

    with scope("prep0"):
        own_k[0:tok, :] = k_ref[:, cols(rank, share)]
        own_v[:, 0:HD, 0:tok] = values_t[rank]
        arrange(0, lambda x: q_ref[:, cols(rank * tiles + x, LANES)])
    with scope("own0"):
        run(groups_of([0], own_k, own_v, slice(0, tok), True), 2, {})
    for copy in mate_k_copies[1:]:
        copy.start()
    hear(0)

    with scope("w_own"):
        for copy in own_k_copies + own_q_copies + own_v_copies:
            copy.wait_recv()
    for copy in mate_v_copies[:1]:
        copy.start()
    with scope("prep1"):
        for slot in range(1, ranks):
            arrange(slot, lambda x: q_all[slot, :, x * LANES:(x + 1) * LANES])

    def relay(name, arrivals, onward):
        with scope(name):
            for copy in arrivals:
                copy.wait_recv()

        @pl.when(has_next)
        def _():
            start_all(onward)

    with scope("own1"):
        run(groups_of(range(1, ranks), own_k, own_v, slice(0, BLOCK), True)
            + groups_of([0], own_k, own_v, slice(tok, BLOCK), False), 2,
            {0: lambda: start_all(mate_v_copies[1:] + fine_copies),
             1: lambda: hear(1),
             3: share_coarse,
             5: lambda: relay("w_mk0", mate_k_copies[:1], relay_k_copies[:1])})

    relay("w_mk1", mate_k_copies[1:], relay_k_copies[1:])
    order = list(range(1, ranks)) + [0]
    mate_groups = groups_of(range(ranks), mate_k, mate_v, slice(0, BLOCK), False)
    with scope("mate"):
        run(mate_groups, len(mate_groups) + 1, {
            len(mate_groups) - 2: lambda: relay("w_mv0", mate_v_copies[:1], relay_v_copies[:1]),
            len(mate_groups) - 1: lambda: relay("w_mv1", mate_v_copies[1:], relay_v_copies[1:])})
    @pl.when(has_other)
    def _():
        with scope("w_other"):
            for copy in relay_k_copies:
                copy.wait_recv()

        with scope("other"):
            run(groups_of(order, other_k, other_v, slice(0, BLOCK), False), None, {})

    with scope("w_outer"):
        for copy in outer_copies:
            copy.wait_recv()
    with scope("far"):
        far = fine_amount + coarse_amount
        k_far = coarse_all[:, 0:coarse_group, :].reshape(coarse_amount, share)
        v_far = coarse_all[:, coarse_group:, :].reshape(coarse_amount, share)
        if use_fine:
            for copy in fine_copies:
                copy.wait_recv()
            fine_rows = fine_all[...].reshape(fine_amount, 2 * share).astype(F32)
            k_far = jnp.concatenate([fine_rows[:, :share], k_far], axis=0)
            v_far = jnp.concatenate([fine_rows[:, share:], v_far], axis=0)

        def reachable(shape, axis):
            spot = lax.broadcasted_iota(jnp.int32, shape, axis)
            fine_pos = o_me * group_tok + spot * FINE
            coarse_pos = (spot - fine_amount) * COARSE
            position = jnp.where(spot < fine_amount, fine_pos, coarse_pos)
            distance = jnp.abs(lax.div(position, BLOCK) - block)
            outside = (spot < fine_amount) | (lax.div(position, group_tok) != o_me)
            return (distance > 1) & outside

        stand_in = own_k[0:16, :].astype(F32)[0:1, :]
        far_k[...] = jnp.where(
            reachable((far, share), 0), k_far, jnp.broadcast_to(stand_in, (far, share))).astype(BF16)
        open_cols = reachable((HD, far), 1)
        turned = v_far.T
        for x in range(kv_local):
            far_v[x, 0:HD, :] = jnp.where(
                open_cols, turned[x * HD:(x + 1) * HD, :], 0.0).astype(BF16)
            far_v[x, HD:, :] = open_cols[0:ONES].astype(F32).astype(BF16)

    def att_copy(part, at):
        device, _ = at_rank(block, part)
        slot = ranks - part - 1
        span = pl.ds(at * UNITS * HD, UNITS * HD)
        return remote(att_send.at[part - 1, span], got_ref.at[slot, span],
                      att_ss.at[slot, at], att_rs.at[slot, at], device)

    per_part = heads // UNITS
    with scope("farrun"):
        run(groups_of(order, far_k, far_v, slice(0, far), False), None, {}, far_weights, far_decays)

    def finish(with_other):
        for part in order:
            for at in range(per_part):
                for head in range(at * UNITS, (at + 1) * UNITS):
                    unit = part * heads + head
                    g = head // heads_kv
                    total = sums[unit]
                    if with_other:
                        total = total * decay_now[unit] + product(unit, other_v[g], weight_ref)
                    total = total * far_decays[unit] + product(unit, far_v[g], far_weights)
                    attended = total[0:HD] / total[HD:HD + 1]
                    rows = slice(head * HD, (head + 1) * HD)
                    if part:
                        att_send[part - 1, rows, :] = attended.astype(BF16)
                    else:
                        out_ref[rows, :] = attended
                if part:
                    att_copy(part, at).start()

    @pl.when(has_other)
    def _():
        with scope("w_otherv"):
            for copy in relay_v_copies:
                copy.wait_recv()
        with scope("fin"):
            finish(True)

    @pl.when(jnp.logical_not(has_other))
    def _():
        with scope("fin"):
            finish(False)

    with scope("w_att"):
        for part in range(1, ranks):
            for at in range(per_part):
                att_copy(part, at).wait_recv()

    with scope("w_send"):
        for copy in (own_k_copies + own_q_copies + own_v_copies + mate_k_copies + mate_v_copies
                     + group_copies + fine_copies + outer_copies):
            copy.wait_send()

        @pl.when(has_next)
        def _():
            for copy in relay_k_copies + relay_v_copies:
                copy.wait_send()

        for part in range(1, ranks):
            for at in range(per_part):
                att_copy(part, at).wait_send()


def norm_kernel(kept_ref, got_ref, gain_ref, out_ref):
    parts = got_ref.shape[0] + 1
    width = kept_ref.shape[0]
    rank = lax.rem(lax.axis_index("inner"), parts)
    blocks = [kept_ref[...]] + [got_ref[n].astype(F32) for n in range(parts - 1)]
    total = sum(jnp.sum(x * x, axis=0, keepdims=True) for x in blocks)
    rescale = lax.rsqrt(total / (parts * width) + EPSILON)
    for n, x in enumerate(blocks):
        column = lax.rem(rank + n, parts)
        cols = pl.ds(pl.multiple_of(column * width, LANES), width)
        out_ref[:, cols] = ((x * rescale).T * gain_ref[:, cols]).astype(BF16)


def local(outer_count, inner_count, queries, keys, values, pool_fine, pool_coarse, gain):
    tok = queries.shape[0]
    ranks = BLOCK // tok
    share = KVH * HD // ranks
    kv_local = share // HD
    q_share = HQ * HD // ranks
    heads = q_share // HD
    group_tok = tok * inner_count
    use_fine = group_tok > 2 * BLOCK
    far = (group_tok // FINE if use_fine else 0) + outer_count * group_tok // COARSE
    coarse_dev = tok // COARSE
    padded = -(-2 * coarse_dev // 8) * 8
    assert ranks >= 2 and BLOCK % tok == 0 and kv_local == 2 and share == LANES
    assert inner_count % (2 * ranks) == 0 and outer_count % 2 == 0
    dma = pltpu.SemaphoreType.DMA
    vmem = pltpu.VMEM
    units = ranks * heads
    pair = lambda: dma((2, ranks))
    k_set = lambda amount: vmem((amount, share), BF16)
    v_set = lambda amount: vmem((kv_local, HD + ONES, amount), BF16)
    line = lambda: vmem((UNITS, 1, tok), F32)
    kept, got = pl.pallas_call(
        functools.partial(kernel, outer_count, inner_count, use_fine),
        out_shape=[jax.ShapeDtypeStruct((q_share, tok), F32),
                   jax.ShapeDtypeStruct((ranks - 1, q_share, tok), BF16)],
        in_specs=[pl.BlockSpec(memory_space=pltpu.HBM)] * 5,
        out_specs=[pl.BlockSpec(memory_space=pltpu.VMEM)] * 2,
        scratch_shapes=[
            vmem(queries.shape, BF16), vmem(keys.shape, BF16), vmem(values.shape, BF16),
            vmem(pool_fine.shape[::-1], F32), vmem(pool_coarse.shape, F32), dma((5,)),
            vmem((ranks, tok, q_share), BF16),
            vmem((units, share, tok), BF16),
            vmem((ranks, kv_local, HD, tok), BF16),
            k_set(BLOCK), v_set(BLOCK), k_set(BLOCK), v_set(BLOCK),
            k_set(BLOCK), v_set(BLOCK), k_set(far), v_set(far),
            vmem((UNITS, max(BLOCK, far), tok), F32),
            vmem((units, BLOCK, tok), BF16),
            vmem((units, 1, tok), F32),
            vmem((units, HD + ONES, tok), F32),
            line(), line(), vmem((units, 1, tok), F32),
            vmem((units, far, tok), BF16), vmem((units, 1, tok), F32),
            vmem((ranks, tok // FINE, 2 * share), BF16),
            vmem((inner_count, tok // FINE, 2 * share), BF16),
            vmem((ranks, padded, share), F32),
            vmem((inner_count, padded, share), F32),
            vmem((outer_count, 2 * inner_count * coarse_dev, share), F32),
            vmem((ranks - 1, q_share, tok), BF16),
            dma((ranks,)), dma((ranks,)),
            pair(), pair(), pair(), pair(), pair(), pair(),
            dma((inner_count - 1,)), dma((inner_count - 1,)),
            dma((inner_count - 1,)), dma((inner_count - 1,)),
            dma((outer_count - 1,)), dma((outer_count - 1,)),
            dma((ranks - 1, heads // UNITS)), dma((ranks - 1, heads // UNITS)),
            pltpu.SemaphoreType.REGULAR((max(outer_count // 2 - 1, 1),)),
        ],
        compiler_params=pltpu.CompilerParams(
            collective_id=0, has_side_effects=True, vmem_limit_bytes=48 * 1024 * 1024),
    )(*(pltpu.with_memory_space_constraint(array, pltpu.HBM) for array in (
        queries, keys, values, pool_fine.T, pool_coarse)))
    return pl.pallas_call(
        norm_kernel,
        out_shape=jax.ShapeDtypeStruct((tok, HQ * HD), BF16),
        in_specs=[pl.BlockSpec(memory_space=pltpu.VMEM)] * 3,
        out_specs=pl.BlockSpec(memory_space=pltpu.VMEM),
        compiler_params=pltpu.CompilerParams(vmem_limit_bytes=8 * 1024 * 1024),
    )(kept, got, gain.reshape(1, -1))


def solution(mesh):
    rows = P(("outer", "inner"), None)
    return jax.shard_map(
        functools.partial(local, mesh.shape["outer"], mesh.shape["inner"]),
        mesh=mesh, in_specs=(rows, rows, rows, P(), P(), P()),
        out_specs=rows, check_vma=False,
    )
```
